64 devices in a mesh: rep: 4 (over x, y), dp: 16 (over z, core).
Axes of the slice: x: 2, y: 2, z: 8, core: 2. Of those that a mesh axis runs over, the one named last changes fastest.
The devices are a block of a 4x4x8 slice.
Arguments:
- g_w_gate: bfloat16 [64, 2, 896, 3584], P(('rep', 'dp')), parts along dimension 0
- g_w_up: bfloat16 [64, 2, 896, 3584], P(('rep', 'dp')), parts along dimension 0
- g_w_down: bfloat16 [64, 2, 3584, 896], P(('rep', 'dp')), parts along dimension 0
- w_gate: bfloat16 [2, 896, 3584], replicated
- w_up: bfloat16 [2, 896, 3584], replicated
- w_down: bfloat16 [2, 3584, 896], replicated
- m_w_gate: float32 [2, 896, 3584], P(None, 'dp')
- m_w_up: float32 [2, 896, 3584], P(None, 'dp')
- m_w_down: float32 [2, 3584, 896], P(None, 'dp')
- v_w_gate: float32 [2, 896, 3584], P(None, 'dp')
- v_w_up: float32 [2, 896, 3584], P(None, 'dp')
- v_w_down: float32 [2, 3584, 896], P(None, 'dp')
Outputs:
- output 1: bfloat16 [8, 896, 3584], P('rep'), parts along dimension 0
- output 2: bfloat16 [8, 896, 3584], P('rep'), parts along dimension 0
- output 3: bfloat16 [8, 3584, 896], P('rep'), parts along dimension 0
- output 4: float32 [8, 896, 3584], P('rep', 'dp'), parts along dimension 0
- output 5: float32 [8, 896, 3584], P('rep', 'dp'), parts along dimension 0
- output 6: float32 [8, 3584, 896], P('rep', 'dp'), parts along dimension 0
- output 7: float32 [8, 896, 3584], P('rep', 'dp'), parts along dimension 0
- output 8: float32 [8, 896, 3584], P('rep', 'dp'), parts along dimension 0
- output 9: float32 [8, 3584, 896], P('rep', 'dp'), parts along dimension 0
There are 4 independent parts. The reference program is written for one: setup_inputs(seed, part) draws one part's arguments, and reference() takes and returns one part's arrays. A program takes and returns all parts, laid end to end along the dimension named above; an argument that names none is the same for every part.
All inputs are finite; a program needn't handle non-finite values.
Results may differ from the reference program's by a relative error of at most 0.022.
Values are sent between devices in bfloat16 or wider.
A program may use at most 768 MiB of HBM per device.

```python
import jax
import jax.numpy as jnp
from jax import lax

DEVICES = 16
D = 896
FF = 3584
LAYERS = 2
NAMES = ("w_gate", "w_up", "w_down")
SHAPES = {"w_gate": (LAYERS, D, FF), "w_up": (LAYERS, D, FF), "w_down": (LAYERS, FF, D)}


def setup_inputs(seed: int = 0, part: int = 0) -> dict:
    kz, *keys = jax.random.split(jax.random.key(seed), 1 + 5 * len(NAMES))
    loud = 2.0 ** jax.random.uniform(kz, (), jnp.float32, -1.0, 1.0)
    drawn = {}
    for name, key, both in zip(NAMES, keys[:3], keys[3:6], strict=True):
        own = jax.random.normal(jax.random.fold_in(key, part), (DEVICES, *SHAPES[name]), jnp.float32)
        shared = jax.random.normal(jax.random.fold_in(both, part), SHAPES[name], jnp.float32)
        drawn["g_" + name] = (loud * (0.7 * shared / DEVICES + 0.7 * own * DEVICES**-0.5)).astype(jnp.bfloat16)
    for name, key in zip(NAMES, keys[6:9], strict=True):
        drawn[name] = (jax.random.normal(key, SHAPES[name], jnp.float32) * SHAPES[name][1] ** -0.5).astype(jnp.bfloat16)
    for name, key in zip(NAMES, keys[9:12], strict=True):
        drawn["m_" + name] = loud * 0.5 * jax.random.normal(key, SHAPES[name], jnp.float32)
    for name, key in zip(NAMES, keys[12:15], strict=True):
        drawn["v_" + name] = loud * loud * jax.random.uniform(key, SHAPES[name], jnp.float32, 0.5, 1.5)
    return drawn


def adamw(w, m, v, g):
    m = 0.9 * m + 0.1 * g
    v = 0.95 * v + 0.05 * g * g
    step = m * lax.rsqrt(v + 1e-8) + 0.1 * w
    return (w - 0.02 * step).astype(jnp.bfloat16), m, v


def clipped(gradients, sum_of_squares, count):
    factor = jnp.minimum(1.0, 0.5 * lax.rsqrt(sum_of_squares / count + 1e-30))
    return [g * factor for g in gradients]


def reference(g_w_gate, g_w_up, g_w_down, w_gate, w_up, w_down, m_w_gate, m_w_up, m_w_down, v_w_gate, v_w_up, v_w_down):
    def total(terms):
        return lax.scan(lambda so_far, term: (so_far + term.astype(jnp.float32), None), jnp.zeros(terms.shape[1:], jnp.float32), terms)[0]

    gradients = [total(terms).astype(jnp.bfloat16).astype(jnp.float32) for terms in (g_w_gate, g_w_up, g_w_down)]
    gradients = clipped(gradients, sum(jnp.sum(g * g) for g in gradients), sum(g.size for g in gradients))
    new = [
        adamw(w.astype(jnp.float32), m, v, g)
        for w, m, v, g in zip((w_gate, w_up, w_down), (m_w_gate, m_w_up, m_w_down), (v_w_gate, v_w_up, v_w_down), gradients, strict=True)
    ]
    return tuple(one[which] for which in range(3) for one in new)
```

```python
import functools
import math

import jax
import jax.numpy as jnp
from jax import lax
from jax.experimental import pallas as pl
from jax.experimental.pallas import tpu as pltpu
from jax.sharding import PartitionSpec as P

MESH = pl.DeviceIdType.MESH
CORES = 2
ROWS, LANES = 8, 128
SLAB = 28
F32 = jnp.float32


def adamw(w, m, v, g):
    m = 0.9 * m + 0.1 * g
    v = 0.95 * v + 0.05 * g * g
    step = m * lax.rsqrt(v + 1e-8) + 0.1 * w
    return (w - 0.02 * step).astype(jnp.bfloat16), m, v


def slabs(ref, body, start=None):
    tiles, columns = ref.shape[0], ref.shape[2]
    size = math.gcd(tiles, max(1, SLAB * LANES // columns))
    return lax.fori_loop(0, tiles // size, lambda i, so_far: body(pl.ds(i * size, size), so_far), start)


def kernel(*refs):
    terms, weights, m_in, v_in, whole, m, v, own, g, w, (squares, pair_send, pair_recv, ring_send, ring_recv, own_sem, load_sem, norm_send, norm_recv) = (
        *(refs[i : i + 3] for i in range(0, 30, 3)),
        refs[30:],
    )
    layers, group = whole[0].shape[:2]
    chips = group // CORES
    count = group * sum(math.prod(one.shape) for one in g)
    me = lax.axis_index("dp")
    core, z = lax.rem(me, CORES), lax.div(me, CORES)
    partner = z * CORES + (1 - core)
    chunks = [(i, l) for i in range(3) for l in range(layers)]

    def away(l, steps):
        return lax.rem(z + (steps if l % 2 == 0 else chips - steps), chips)

    def come(l, steps):
        return lax.rem(z + (chips - steps if l % 2 == 0 else steps), chips)

    def remote(src, dst, send, recv, device):
        return pltpu.make_async_remote_copy(src_ref=src, dst_ref=dst, send_sem=send, recv_sem=recv, device_id={"dp": device}, device_id_type=MESH)

    def pair(i, l, s):
        return remote(terms[i].at[l, come(l, s + 1) * CORES + (1 - core)], whole[i].at[l, s], pair_send.at[i, l, s], pair_recv.at[i, l, s], partner)

    def mine(i, l, s):
        return pltpu.make_async_copy(terms[i].at[l, come(l, s + 1) * CORES + core], own[i].at[lax.rem(s, 2), l], own_sem.at[i, l, lax.rem(s, 2)])

    def total(l, s):
        return chips + s - 1

    def send_total(i, l, s):
        src = s if isinstance(s, int) and s == 0 else total(l, s)
        return remote(whole[i].at[l, src], whole[i].at[l, total(l, s + 1)], ring_send.at[i, l, s], ring_recv.at[i, l, s], away(l, 1) * CORES + core)

    def add(i, l, s, first, last):
        if not first:
            send_total(i, l, s - 1).wait_recv()
        mine(i, l, s).wait()
        pair(i, l, s).wait_recv()

        def body(at, so_far):
            value = own[i][lax.rem(s, 2), l, at].astype(F32) + whole[i][l, s, at].astype(F32)
            if not first:
                value += whole[i][l, total(l, s), at].astype(F32)
            value = value.astype(jnp.bfloat16)
            if not last:
                whole[i][l, s if first else total(l, s), at] = value
                return so_far
            g[i][l, at] = value
            value = value.astype(F32)
            value = jnp.sum(value * value, axis=0)
            for column in range(0, value.shape[1], LANES):
                so_far += value[:, column : column + LANES]
            return so_far

        return slabs(g[i].at[l], body, jnp.zeros((ROWS, LANES), F32) if last else None)

    for i, l in chunks:
        mine(i, l, 0).start()
    barrier = pltpu.get_barrier_semaphore()
    for other in range(1, group):
        pl.semaphore_signal(barrier, inc=1, device_id={"dp": lax.rem(me + other, group)}, device_id_type=MESH)
    pl.semaphore_wait(barrier, group - 1)
    for s in range(2):
        for i, l in chunks:
            pair(i, l, s).start()

    def loads():
        for i in range(3):
            yield pltpu.make_async_copy(m_in[i], m[i], load_sem.at[i, 0])
            yield pltpu.make_async_copy(v_in[i], v[i], load_sem.at[i, 1])
            for l in range(layers):
                yield pltpu.make_async_copy(weights[i].at[l, me], w[i].at[l], load_sem.at[i, 2 + l])

    def step(s, first):
        for i, l in chunks:
            mine(i, l, s + 1).start()
        for i, l in chunks:
            add(i, l, s, first, False)
            send_total(i, l, s).start()

    step(0, True)
    for load in loads():
        load.start()

    @pl.loop(1, chips - 1)
    def _(s):
        for i, l in chunks:
            pair(i, l, s + 1).start()
        step(s, False)

    square = jnp.zeros((ROWS, LANES), F32)
    for i, l in chunks:
        square += add(i, l, chips - 1, False, True)
    squares[me] = square

    @pl.loop(0, chips)
    def _(s):
        for i, l in chunks:
            pair(i, l, s).wait_send()

    send_wait = lambda i, l, s: remote(whole[i].at[l, s], whole[i].at[l, s], ring_send.at[i, l, s], ring_recv.at[i, l, s], away(l, 1) * CORES + core).wait_send()

    @pl.loop(0, chips - 1)
    def _(s):
        for i, l in chunks:
            send_wait(i, l, s)

    def norm(to, source):
        return remote(squares.at[source], squares.at[source], norm_send.at[to], norm_recv.at[source], to)

    for other in range(1, group):
        norm(lax.rem(me + other, group), me).start()
    for load in loads():
        load.wait()
    for other in range(1, group):
        norm(lax.rem(me + other, group), lax.rem(me + other, group)).wait_recv()
    square = jnp.sum(jnp.sum(squares[...], axis=0), axis=(0, 1), keepdims=True)
    factor = jnp.minimum(1.0, 0.5 * lax.rsqrt(square / count + 1e-30))[None]

    def ring(i, l, s):
        slot = whole[i].at[l, come(l, s) * CORES + core]
        return remote(slot, slot, ring_send.at[i, l, s], ring_recv.at[i, l, s], away(l, 1) * CORES + core)

    def share(i, l, s):
        slot = whole[i].at[l, come(l, s) * CORES + core]
        return remote(slot, slot, pair_send.at[i, l, s], pair_recv.at[i, l, s], partner)

    for i, l in chunks:

        def body(at, so_far):
            new = adamw(w[i][l, at].astype(F32), m[i][l, at], v[i][l, at], g[i][l, at].astype(F32) * factor)
            whole[i][l, me, at], m[i][l, at], v[i][l, at] = new
            return so_far

        slabs(g[i].at[l], body)
        ring(i, l, 0).start()
        share(i, l, 0).start()

    @pl.loop(1, chips - 1)
    def _(s):
        for i, l in chunks:
            ring(i, l, s - 1).wait_recv()
            ring(i, l, s).start()
            share(i, l, s).start()

    for i, l in chunks:
        ring(i, l, chips - 2).wait_recv()
        share(i, l, chips - 1).start()

    for other in range(1, group):
        norm(lax.rem(me + other, group), me).wait_send()

    @pl.loop(0, chips - 1)
    def _(s):
        for i, l in chunks:
            ring(i, l, s).wait_send()

    @pl.loop(0, chips)
    def _(s):
        for i, l in chunks:
            share(i, l, s).wait_send()
            share(i, l, s).wait_recv()


def write(*refs):
    half = (len(refs) - 1) // 2
    copies = [pltpu.make_async_copy(src, dst, refs[-1].at[i]) for i, (src, dst) in enumerate(zip(refs[:half], refs[half : 2 * half], strict=True))]
    for copy in copies:
        copy.start()
    for copy in copies:
        copy.wait()


def solution(mesh):
    group = mesh.shape["dp"]
    chips = group // CORES

    def step(*arrays):
        terms, weights, m, v = (arrays[i : i + 3] for i in (0, 3, 6, 9))
        layers = terms[0].shape[1]
        chunk = [(one.shape[1] // ROWS, ROWS, one.shape[2]) for one in m]
        blocks = [(layers, group, *one) for one in chunk]
        local = [(layers, *one) for one in chunk]
        terms = [one.reshape(shape) for one, shape in zip(terms, blocks, strict=True)]
        old = [one.reshape(shape) for one, shape in zip(weights, blocks, strict=True)]
        moments = [one.reshape(shape) for one, shape in zip(m + v, local * 2, strict=True)]
        kept = [pltpu.VMEM(shape, jnp.bfloat16) for shape in blocks] + [pltpu.VMEM(shape, F32) for shape in local * 2]
        elements = sum(math.prod(shape) for shape in blocks)
        new = pl.pallas_call(
            kernel,
            out_shape=kept,
            in_specs=[pl.BlockSpec(memory_space=pltpu.HBM)] * 12,
            out_specs=[pl.BlockSpec(memory_space=pltpu.VMEM)] * 9,
            scratch_shapes=[
                *(pltpu.VMEM((2, *shape), jnp.bfloat16) for shape in local),
                *(pltpu.VMEM(shape, jnp.bfloat16) for shape in local * 2),
                pltpu.VMEM((group, ROWS, LANES), F32),
                *[pltpu.SemaphoreType.DMA((3, layers, chips))] * 4,
                pltpu.SemaphoreType.DMA((3, layers, 2)),
                pltpu.SemaphoreType.DMA((3, 2 + layers)),
                *[pltpu.SemaphoreType.DMA((group,))] * 2,
            ],
            compiler_params=pltpu.CompilerParams(collective_id=0, has_side_effects=True, vmem_limit_bytes=12 * 2**20),
            cost_estimate=pl.CostEstimate(flops=20 * elements, bytes_accessed=4 * elements, transcendentals=elements // group),
        )(*terms, *old, *moments)
        out = pl.pallas_call(
            write,
            out_shape=[jax.ShapeDtypeStruct(one.shape, one.dtype) for one in new],
            in_specs=[pl.BlockSpec(memory_space=pl.ANY)] * 9,
            out_specs=[pl.BlockSpec(memory_space=pl.ANY)] * 9,
            scratch_shapes=[pltpu.SemaphoreType.DMA((9,))],
            compiler_params=pltpu.CompilerParams(vmem_limit_bytes=12 * 2**20, has_side_effects=True),
        )(*new)
        return tuple(one.reshape(like.shape) for one, like in zip(out, weights + m + v, strict=True))

    all_of, cut = P(None, None, None), P(None, "dp", None)
    return jax.shard_map(
        step,
        mesh=mesh,
        in_specs=(P(("rep", "dp"), None, None, None),) * 3 + (all_of,) * 3 + (cut,) * 6,
        out_specs=(P("rep", None, None),) * 3 + (P("rep", "dp", None),) * 6,
        check_vma=False,
    )
```

```python
import functools
import math

import jax
import jax.numpy as jnp
from jax import lax
from jax.experimental import pallas as pl
from jax.experimental.pallas import tpu as pltpu
from jax.sharding import PartitionSpec as P

MESH = pl.DeviceIdType.MESH
CORES = 2
ROWS, LANES = 8, 128
SLAB = 28
F32 = jnp.float32


def adamw(w, m, v, g):
    m = 0.9 * m + 0.1 * g
    v = 0.95 * v + 0.05 * g * g
    step = m * lax.rsqrt(v + 1e-8) + 0.1 * w
    return (w - 0.02 * step).astype(jnp.bfloat16), m, v


def slabs(ref, body, start=None):
    tiles, columns = ref.shape[0], ref.shape[2]
    size = math.gcd(tiles, max(1, SLAB * LANES // columns))
    return lax.fori_loop(0, tiles // size, lambda i, so_far: body(pl.ds(i * size, size), so_far), start)


def kernel(*refs):
    layers = refs[0].shape[0]
    inputs, flat, rest = refs[:12], refs[12 : 12 + 3 * layers], refs[12 + 3 * layers :]
    terms, weights, m_in, v_in = (inputs[i : i + 3] for i in range(0, 12, 3))
    whole = [flat[i : i + layers] for i in range(0, 3 * layers, layers)]
    m, v, own = (rest[i : i + 3] for i in range(0, 9, 3))
    squares, pair_send, pair_recv, ring_send, ring_recv, own_sem, load_sem, norm_send, norm_recv = rest[9:]
    group = terms[0].shape[1]
    chips = group // CORES
    count = group * sum(math.prod(one.shape) for one in m)
    end = (chips - 1) % 2
    g, w = ([one.at[slot] for one in own] for slot in (end, 1 - end))
    me = lax.axis_index("dp")
    core, z = lax.rem(me, CORES), lax.div(me, CORES)
    partner = z * CORES + (1 - core)
    chunks = [(i, l) for i in range(3) for l in range(layers)]

    def away(l, steps):
        return lax.rem(z + (steps if l % 2 == 0 else chips - steps), chips)

    def come(l, steps):
        return lax.rem(z + (chips - steps if l % 2 == 0 else steps), chips)

    def remote(src, dst, send, recv, device):
        return pltpu.make_async_remote_copy(src_ref=src, dst_ref=dst, send_sem=send, recv_sem=recv, device_id={"dp": device}, device_id_type=MESH)

    def pair(i, l, s):
        return remote(terms[i].at[l, come(l, s + 1) * CORES + (1 - core)], whole[i][l].at[s], pair_send.at[i, l, s], pair_recv.at[i, l, s], partner)

    def mine(i, l, s):
        return pltpu.make_async_copy(terms[i].at[l, come(l, s + 1) * CORES + core], own[i].at[lax.rem(s, 2), l], own_sem.at[i, l, lax.rem(s, 2)])

    def total(l, s):
        return chips + s - 1

    def send_total(i, l, s):
        src = s if isinstance(s, int) and s == 0 else total(l, s)
        return remote(whole[i][l].at[src], whole[i][l].at[total(l, s + 1)], ring_send.at[i, l, s], ring_recv.at[i, l, s], away(l, 1) * CORES + core)

    def add(i, l, s, first, last):
        if not first:
            send_total(i, l, s - 1).wait_recv()
        mine(i, l, s).wait()
        pair(i, l, s).wait_recv()

        def body(at, so_far):
            value = own[i][lax.rem(s, 2), l, at].astype(F32) + whole[i][l][s, at].astype(F32)
            if not first:
                value += whole[i][l][total(l, s), at].astype(F32)
            value = value.astype(jnp.bfloat16)
            if not last:
                whole[i][l][s if first else total(l, s), at] = value
                return so_far
            g[i][l, at] = value
            value = value.astype(F32)
            value = jnp.sum(value * value, axis=0)
            for column in range(0, value.shape[1], LANES):
                so_far += value[:, column : column + LANES]
            return so_far

        return slabs(m[i].at[l], body, jnp.zeros((ROWS, LANES), F32) if last else None)

    for i, l in chunks:
        mine(i, l, 0).start()
    barrier = pltpu.get_barrier_semaphore()
    for other in range(1, group):
        pl.semaphore_signal(barrier, inc=1, device_id={"dp": lax.rem(me + other, group)}, device_id_type=MESH)
    pl.semaphore_wait(barrier, group - 1)
    for s in range(2):
        for i, l in chunks:
            pair(i, l, s).start()

    moments = [pltpu.make_async_copy(src[i], dst[i], load_sem.at[i, k]) for i in range(3) for k, (src, dst) in enumerate(((m_in, m), (v_in, v)))]
    old = [pltpu.make_async_copy(weights[i].at[l, me], w[i].at[l], load_sem.at[i, 2 + l]) for i, l in chunks]

    def step(s, first):
        for i, l in chunks:
            mine(i, l, s + 1).start()
        for i, l in chunks:
            add(i, l, s, first, False)
            send_total(i, l, s).start()

    step(0, True)
    for load in moments:
        load.start()

    @pl.loop(1, chips - 1)
    def _(s):
        for i, l in chunks:
            pair(i, l, s + 1).start()
        step(s, False)

    for load in old:
        load.start()
    square = jnp.zeros((ROWS, LANES), F32)
    for i, l in chunks:
        square += add(i, l, chips - 1, False, True)
    squares[me] = square

    @pl.loop(0, chips)
    def _(s):
        for i, l in chunks:
            pair(i, l, s).wait_send()

    send_wait = lambda i, l, s: remote(whole[i][l].at[s], whole[i][l].at[s], ring_send.at[i, l, s], ring_recv.at[i, l, s], away(l, 1) * CORES + core).wait_send()

    @pl.loop(0, chips - 1)
    def _(s):
        for i, l in chunks:
            send_wait(i, l, s)

    def norm(to, source):
        return remote(squares.at[source], squares.at[source], norm_send.at[to], norm_recv.at[source], to)

    for other in range(1, group):
        norm(lax.rem(me + other, group), me).start()
    for load in (*moments, *old):
        load.wait()
    for other in range(1, group):
        norm(lax.rem(me + other, group), lax.rem(me + other, group)).wait_recv()
    square = jnp.sum(jnp.sum(squares[...], axis=0), axis=(0, 1), keepdims=True)
    factor = jnp.minimum(1.0, 0.5 * lax.rsqrt(square / count + 1e-30))[None]

    def ring(i, l, s):
        slot = whole[i][l].at[come(l, s) * CORES + core]
        return remote(slot, slot, ring_send.at[i, l, s], ring_recv.at[i, l, s], away(l, 1) * CORES + core)

    def share(i, l, s):
        slot = whole[i][l].at[come(l, s) * CORES + core]
        return remote(slot, slot, pair_send.at[i, l, s], pair_recv.at[i, l, s], partner)

    for i, l in chunks:

        def body(at, so_far):
            new = adamw(w[i][l, at].astype(F32), m[i][l, at], v[i][l, at], g[i][l, at].astype(F32) * factor)
            whole[i][l][me, at], m[i][l, at], v[i][l, at] = new
            return so_far

        slabs(m[i].at[l], body)
        ring(i, l, 0).start()
        share(i, l, 0).start()

    @pl.loop(1, chips - 1)
    def _(s):
        for i, l in chunks:
            ring(i, l, s - 1).wait_recv()
            ring(i, l, s).start()
            share(i, l, s).start()

    for i, l in chunks:
        ring(i, l, chips - 2).wait_recv()
        share(i, l, chips - 1).start()

    for other in range(1, group):
        norm(lax.rem(me + other, group), me).wait_send()

    @pl.loop(0, chips - 1)
    def _(s):
        for i, l in chunks:
            ring(i, l, s).wait_send()

    @pl.loop(0, chips)
    def _(s):
        for i, l in chunks:
            share(i, l, s).wait_send()
            share(i, l, s).wait_recv()


def write(layers, *refs):
    *refs, sem = refs
    src, dst = refs[:-9], refs[-9:]
    pieces = [(src[i * layers + l], dst[i].at[l]) for i in range(3) for l in range(layers)]
    pieces += zip(src[3 * layers :], dst[3:], strict=True)
    copies = [pltpu.make_async_copy(*piece, sem.at[i]) for i, piece in enumerate(pieces)]
    for copy in copies:
        copy.start()
    for copy in copies:
        copy.wait()


def solution(mesh):
    group = mesh.shape["dp"]
    chips = group // CORES

    def step(*arrays):
        terms, weights, m, v = (arrays[i : i + 3] for i in (0, 3, 6, 9))
        layers = terms[0].shape[1]
        chunk = [(one.shape[1] // ROWS, ROWS, one.shape[2]) for one in m]
        blocks = [(layers, group, *one) for one in chunk]
        local = [(layers, *one) for one in chunk]
        terms = [one.reshape(shape) for one, shape in zip(terms, blocks, strict=True)]
        old = [one.reshape(shape) for one, shape in zip(weights, blocks, strict=True)]
        moments = [one.reshape(shape) for one, shape in zip(m + v, local * 2, strict=True)]
        kept = [pltpu.VMEM(shape[1:], jnp.bfloat16) for shape in blocks for _ in range(layers)] + [pltpu.VMEM(shape, F32) for shape in local * 2]
        elements = sum(math.prod(shape) for shape in blocks)
        new = pl.pallas_call(
            kernel,
            out_shape=kept,
            in_specs=[pl.BlockSpec(memory_space=pltpu.HBM)] * 12,
            out_specs=[pl.BlockSpec(memory_space=pltpu.VMEM)] * len(kept),
            scratch_shapes=[
                *(pltpu.VMEM((2, *shape), jnp.bfloat16) for shape in local),
                pltpu.VMEM((group, ROWS, LANES), F32),
                *[pltpu.SemaphoreType.DMA((3, layers, chips))] * 4,
                pltpu.SemaphoreType.DMA((3, layers, 2)),
                pltpu.SemaphoreType.DMA((3, 2 + layers)),
                *[pltpu.SemaphoreType.DMA((group,))] * 2,
            ],
            compiler_params=pltpu.CompilerParams(collective_id=0, has_side_effects=True, vmem_limit_bytes=8 * 2**20),
            cost_estimate=pl.CostEstimate(flops=20 * elements, bytes_accessed=4 * elements, transcendentals=elements // group),
        )(*terms, *old, *moments)
        out = pl.pallas_call(
            functools.partial(write, layers),
            out_shape=[jax.ShapeDtypeStruct(shape, jnp.bfloat16) for shape in blocks] + [jax.ShapeDtypeStruct(shape, F32) for shape in local * 2],
            in_specs=[pl.BlockSpec(memory_space=pl.ANY)] * len(kept),
            out_specs=[pl.BlockSpec(memory_space=pl.ANY)] * 9,
            scratch_shapes=[pltpu.SemaphoreType.DMA((len(kept),))],
            compiler_params=pltpu.CompilerParams(vmem_limit_bytes=8 * 2**20),
        )(*new)
        return tuple(one.reshape(like.shape) for one, like in zip(out, weights + m + v, strict=True))

    all_of, cut = P(None, None, None), P(None, "dp", None)
    return jax.shard_map(
        step,
        mesh=mesh,
        in_specs=(P(("rep", "dp"), None, None, None),) * 3 + (all_of,) * 3 + (cut,) * 6,
        out_specs=(P("rep", None, None),) * 3 + (P("rep", "dp", None),) * 6,
        check_vma=False,
    )
```

```python
import functools
import math

import jax
import jax.numpy as jnp
from jax import lax
from jax.experimental import pallas as pl
from jax.experimental.pallas import tpu as pltpu
from jax.sharding import PartitionSpec as P

MESH = pl.DeviceIdType.MESH
CORES = 2
ROWS, LANES = 8, 128
SLAB = 28
F32 = jnp.float32


def adamw(w, m, v, g):
    m = 0.9 * m + 0.1 * g
    v = 0.95 * v + 0.05 * g * g
    step = m * lax.rsqrt(v + 1e-8) + 0.1 * w
    return (w - 0.02 * step).astype(jnp.bfloat16), m, v


def slabs(ref, body, start=None):
    tiles, columns = ref.shape[0], ref.shape[2]
    size = math.gcd(tiles, max(1, SLAB * LANES // columns))
    return lax.fori_loop(0, tiles // size, lambda i, so_far: body(pl.ds(i * size, size), so_far), start)


def kernel(*refs):
    layers = refs[0].shape[0]
    inputs, flat, rest = refs[:12], refs[12 : 12 + 3 * layers], refs[12 + 3 * layers :]
    terms, weights, m_in, v_in = (inputs[i : i + 3] for i in range(0, 12, 3))
    whole = [flat[i : i + layers] for i in range(0, 3 * layers, layers)]
    m, v, own = (rest[i : i + 3] for i in range(0, 9, 3))
    squares, pair_send, pair_recv, ring_send, ring_recv, own_sem, stage_sem, load_sem, norm_send, norm_recv = rest[9:]
    group = terms[0].shape[1]
    chips = group // CORES
    count = group * sum(math.prod(one.shape) for one in m)
    end = (chips - 1) % 2
    g, w = ([one.at[slot] for one in own] for slot in (end, 1 - end))
    me = lax.axis_index("dp")
    core, z = lax.rem(me, CORES), lax.div(me, CORES)
    partner = z * CORES + (1 - core)
    chunks = [(i, l) for i in range(3) for l in range(layers)]

    def away(l, steps):
        return lax.rem(z + (steps if l % 2 == 0 else chips - steps), chips)

    def come(l, steps):
        return lax.rem(z + (chips - steps if l % 2 == 0 else steps), chips)

    def remote(src, dst, send, recv, device):
        return pltpu.make_async_remote_copy(src_ref=src, dst_ref=dst, send_sem=send, recv_sem=recv, device_id={"dp": device}, device_id_type=MESH)

    def stage(i, l):
        return pltpu.make_async_copy(terms[i].at[l, come(l, 1) * CORES + (1 - core)], whole[i][l].at[group - 1], stage_sem.at[i, l])

    def pair(i, l, s):
        first = isinstance(s, int) and s == 0
        return remote(whole[i][l].at[group - 1] if first else terms[i].at[l, come(l, s + 1) * CORES + (1 - core)], whole[i][l].at[s], pair_send.at[i, l, s], pair_recv.at[i, l, s], partner)

    def mine(i, l, s):
        return pltpu.make_async_copy(terms[i].at[l, come(l, s + 1) * CORES + core], own[i].at[lax.rem(s, 2), l], own_sem.at[i, l, lax.rem(s, 2)])

    def total(l, s):
        return chips + s - 1

    def send_total(i, l, s):
        src = s if isinstance(s, int) and s == 0 else total(l, s)
        return remote(whole[i][l].at[src], whole[i][l].at[total(l, s + 1)], ring_send.at[i, l, s], ring_recv.at[i, l, s], away(l, 1) * CORES + core)

    def add(i, l, s, first, last):
        if not first:
            send_total(i, l, s - 1).wait_recv()
        mine(i, l, s).wait()
        pair(i, l, s).wait_recv()

        def body(at, so_far):
            value = own[i][lax.rem(s, 2), l, at].astype(F32) + whole[i][l][s, at].astype(F32)
            if not first:
                value += whole[i][l][total(l, s), at].astype(F32)
            value = value.astype(jnp.bfloat16)
            if not last:
                whole[i][l][s if first else total(l, s), at] = value
                return so_far
            g[i][l, at] = value
            value = value.astype(F32)
            value = jnp.sum(value * value, axis=0)
            for column in range(0, value.shape[1], LANES):
                so_far += value[:, column : column + LANES]
            return so_far

        return slabs(m[i].at[l], body, jnp.zeros((ROWS, LANES), F32) if last else None)

    for i, l in chunks:
        stage(i, l).start()
        mine(i, l, 0).start()
    barrier = pltpu.get_barrier_semaphore()
    for other in (partner, away(0, 1) * CORES + core, come(0, 1) * CORES + core):
        pl.semaphore_signal(barrier, inc=1, device_id={"dp": other}, device_id_type=MESH)
    pl.semaphore_wait(barrier, 3)
    for i, l in chunks:
        stage(i, l).wait()
        pair(i, l, 0).start()
    for i, l in chunks:
        pair(i, l, 1).start()

    moments = [pltpu.make_async_copy(src[i], dst[i], load_sem.at[i, k]) for i in range(3) for k, (src, dst) in enumerate(((m_in, m), (v_in, v)))]
    old = [pltpu.make_async_copy(weights[i].at[l, me], w[i].at[l], load_sem.at[i, 2 + l]) for i, l in chunks]

    def step(s, first):
        for i, l in chunks:
            mine(i, l, s + 1).start()
        for i, l in chunks:
            add(i, l, s, first, False)
            send_total(i, l, s).start()

    step(0, True)
    for load in moments:
        load.start()

    @pl.loop(1, chips - 1)
    def _(s):
        for i, l in chunks:
            pair(i, l, s + 1).start()
        step(s, False)

    for load in old:
        load.start()

    def sent(i, l, s):
        slot = whole[i][l].at[s]
        return remote(slot, slot, ring_send.at[i, l, s], ring_recv.at[i, l, s], away(l, 1) * CORES + core)

    @pl.loop(0, chips - 2)
    def _(s):
        for i, l in chunks:
            pair(i, l, s).wait_send()
            sent(i, l, s).wait_send()

    for i, l in chunks:
        pair(i, l, chips - 2).wait_send()
    square = jnp.zeros((ROWS, LANES), F32)
    for i, l in chunks:
        square += add(i, l, chips - 1, False, True)
    squares[me] = jnp.sum(square, axis=0, keepdims=True)
    for i, l in chunks:
        pair(i, l, chips - 1).wait_send()
        sent(i, l, chips - 2).wait_send()

    def norm(to, source):
        return remote(squares.at[source], squares.at[source], norm_send.at[to], norm_recv.at[source], to)

    for other in range(1, group):
        norm(lax.rem(me + other, group), me).start()
    for load in (*moments, *old):
        load.wait()
    for other in range(1, group):
        norm(lax.rem(me + other, group), lax.rem(me + other, group)).wait_recv()
    square = jnp.sum(jnp.sum(squares[...], axis=0), axis=1, keepdims=True)
    factor = jnp.minimum(1.0, 0.5 * lax.rsqrt(square / count + 1e-30))[None]

    def ring(i, l, s):
        slot = whole[i][l].at[come(l, s) * CORES + core]
        return remote(slot, slot, ring_send.at[i, l, s], ring_recv.at[i, l, s], away(l, 1) * CORES + core)

    def share(i, l, s):
        slot = whole[i][l].at[come(l, s) * CORES + core]
        return remote(slot, slot, pair_send.at[i, l, s], pair_recv.at[i, l, s], partner)

    for i, l in chunks:

        def body(at, so_far):
            new = adamw(w[i][l, at].astype(F32), m[i][l, at], v[i][l, at], g[i][l, at].astype(F32) * factor)
            whole[i][l][me, at], m[i][l, at], v[i][l, at] = new
            return so_far

        slabs(m[i].at[l], body)
        ring(i, l, 0).start()
        share(i, l, 0).start()

    @pl.loop(1, chips - 1)
    def _(s):
        for i, l in chunks:
            ring(i, l, s - 1).wait_recv()
            ring(i, l, s).start()
            share(i, l, s).start()

    for other in range(1, group):
        norm(lax.rem(me + other, group), me).wait_send()

    @pl.loop(0, chips - 2)
    def _(s):
        for i, l in chunks:
            ring(i, l, s).wait_send()
            share(i, l, s).wait_send()
            share(i, l, s).wait_recv()

    for i, l in chunks:
        ring(i, l, chips - 2).wait_recv()
        share(i, l, chips - 1).start()
    for s in (chips - 2, chips - 1):
        for i, l in chunks:
            if s < chips - 1:
                ring(i, l, s).wait_send()
            share(i, l, s).wait_send()
            share(i, l, s).wait_recv()


def write(layers, *refs):
    *refs, sem = refs
    src, dst = refs[:-9], refs[-9:]
    pieces = [(src[i * layers + l], dst[i].at[l]) for i in range(3) for l in range(layers)]
    pieces += zip(src[3 * layers :], dst[3:], strict=True)
    copies = [pltpu.make_async_copy(*piece, sem.at[i]) for i, piece in enumerate(pieces)]
    for copy in copies:
        copy.start()
    for copy in copies:
        copy.wait()


def solution(mesh):
    group = mesh.shape["dp"]
    chips = group // CORES

    def step(*arrays):
        terms, weights, m, v = (arrays[i : i + 3] for i in (0, 3, 6, 9))
        layers = terms[0].shape[1]
        chunk = [(one.shape[1] // ROWS, ROWS, one.shape[2]) for one in m]
        blocks = [(layers, group, *one) for one in chunk]
        local = [(layers, *one) for one in chunk]
        terms = [one.reshape(shape) for one, shape in zip(terms, blocks, strict=True)]
        old = [one.reshape(shape) for one, shape in zip(weights, blocks, strict=True)]
        moments = [one.reshape(shape) for one, shape in zip(m + v, local * 2, strict=True)]
        kept = [pltpu.VMEM(shape[1:], jnp.bfloat16) for shape in blocks for _ in range(layers)] + [pltpu.VMEM(shape, F32) for shape in local * 2]
        elements = sum(math.prod(shape) for shape in blocks)
        new = pl.pallas_call(
            kernel,
            out_shape=kept,
            in_specs=[pl.BlockSpec(memory_space=pltpu.HBM)] * 12,
            out_specs=[pl.BlockSpec(memory_space=pltpu.VMEM)] * len(kept),
            scratch_shapes=[
                *(pltpu.VMEM((2, *shape), jnp.bfloat16) for shape in local),
                pltpu.VMEM((group, 1, LANES), F32),
                *[pltpu.SemaphoreType.DMA((3, layers, chips))] * 4,
                pltpu.SemaphoreType.DMA((3, layers, 2)),
                pltpu.SemaphoreType.DMA((3, layers)),
                pltpu.SemaphoreType.DMA((3, 2 + layers)),
                *[pltpu.SemaphoreType.DMA((group,))] * 2,
            ],
            compiler_params=pltpu.CompilerParams(collective_id=0, has_side_effects=True, vmem_limit_bytes=8 * 2**20),
            cost_estimate=pl.CostEstimate(flops=20 * elements, bytes_accessed=4 * elements, transcendentals=elements // group),
        )(*terms, *old, *moments)
        out = pl.pallas_call(
            functools.partial(write, layers),
            out_shape=[jax.ShapeDtypeStruct(shape, jnp.bfloat16) for shape in blocks] + [jax.ShapeDtypeStruct(shape, F32) for shape in local * 2],
            in_specs=[pl.BlockSpec(memory_space=pl.ANY)] * len(kept),
            out_specs=[pl.BlockSpec(memory_space=pl.ANY)] * 9,
            scratch_shapes=[pltpu.SemaphoreType.DMA((len(kept),))],
            compiler_params=pltpu.CompilerParams(vmem_limit_bytes=8 * 2**20),
        )(*new)
        return tuple(one.reshape(like.shape) for one, like in zip(out, weights + m + v, strict=True))

    all_of, cut = P(None, None, None), P(None, "dp", None)
    return jax.shard_map(
        step,
        mesh=mesh,
        in_specs=(P(("rep", "dp"), None, None, None),) * 3 + (all_of,) * 3 + (cut,) * 6,
        out_specs=(P("rep", None, None),) * 3 + (P("rep", "dp", None),) * 6,
        check_vma=False,
    )
```

```python
import functools
import math

import jax
import jax.numpy as jnp
from jax import lax
from jax.experimental import pallas as pl
from jax.experimental.pallas import tpu as pltpu
from jax.sharding import PartitionSpec as P

MESH = pl.DeviceIdType.MESH
CORES = 2
ROWS, LANES = 8, 128
SLAB = 28
F32 = jnp.float32


def adamw(w, m, v, g):
    m = 0.9 * m + 0.1 * g
    v = 0.95 * v + 0.05 * g * g
    step = m * lax.rsqrt(v + 1e-8) + 0.1 * w
    return (w - 0.02 * step).astype(jnp.bfloat16), m, v


def slabs(ref, body, start=None):
    tiles, columns = ref.shape[0], ref.shape[2]
    size = math.gcd(tiles, max(1, SLAB * LANES // columns))
    return lax.fori_loop(0, tiles // size, lambda i, so_far: body(pl.ds(i * size, size), so_far), start)


def kernel(*refs):
    layers = refs[0].shape[0]
    inputs, flat, rest = refs[:12], refs[12 : 12 + 3 * layers], refs[12 + 3 * layers :]
    terms, weights, m_in, v_in = (inputs[i : i + 3] for i in range(0, 12, 3))
    whole = [flat[i : i + layers] for i in range(0, 3 * layers, layers)]
    m, v, own = (rest[i : i + 3] for i in range(0, 9, 3))
    squares, pair_send, pair_recv, ring_send, ring_recv, own_sem, stage_sem, load_sem, norm_send, norm_recv = rest[9:]
    group = terms[0].shape[1]
    chips = group // CORES
    count = group * sum(math.prod(one.shape) for one in m)
    end = (chips - 1) % 2
    g, w = ([one.at[slot] for one in own] for slot in (end, 1 - end))
    me = lax.axis_index("dp")
    core, z = lax.rem(me, CORES), lax.div(me, CORES)
    partner = z * CORES + (1 - core)
    chunks = [(i, l) for i in range(3) for l in range(layers)]

    def away(l, steps):
        return lax.rem(z + (steps if l % 2 == 0 else chips - steps), chips)

    def come(l, steps):
        return lax.rem(z + (chips - steps if l % 2 == 0 else steps), chips)

    def remote(src, dst, send, recv, device):
        return pltpu.make_async_remote_copy(src_ref=src, dst_ref=dst, send_sem=send, recv_sem=recv, device_id={"dp": device}, device_id_type=MESH)

    def stage(i, l):
        return pltpu.make_async_copy(terms[i].at[l, come(l, 1) * CORES + (1 - core)], whole[i][l].at[group - 1], stage_sem.at[i, l])

    def pair(i, l, s):
        first = isinstance(s, int) and s == 0
        return remote(whole[i][l].at[group - 1] if first else terms[i].at[l, come(l, s + 1) * CORES + (1 - core)], whole[i][l].at[s], pair_send.at[i, l, s], pair_recv.at[i, l, s], partner)

    def mine(i, l, s):
        return pltpu.make_async_copy(terms[i].at[l, come(l, s + 1) * CORES + core], own[i].at[lax.rem(s, 2), l], own_sem.at[i, l, lax.rem(s, 2)])

    def total(l, s):
        return chips + s - 1

    def send_total(i, l, s):
        src = s if isinstance(s, int) and s == 0 else total(l, s)
        return remote(whole[i][l].at[src], whole[i][l].at[total(l, s + 1)], ring_send.at[i, l, s], ring_recv.at[i, l, s], away(l, 1) * CORES + core)

    def add(i, l, s, first, last):
        if not first:
            send_total(i, l, s - 1).wait_recv()
        mine(i, l, s).wait()
        pair(i, l, s).wait_recv()

        def body(at, so_far):
            value = own[i][lax.rem(s, 2), l, at].astype(F32) + whole[i][l][s, at].astype(F32)
            if not first:
                value += whole[i][l][total(l, s), at].astype(F32)
            value = value.astype(jnp.bfloat16)
            if not last:
                whole[i][l][s if first else total(l, s), at] = value
                return so_far
            g[i][l, at] = value
            value = value.astype(F32)
            value = jnp.sum(value * value, axis=0)
            for column in range(0, value.shape[1], LANES):
                so_far += value[:, column : column + LANES]
            return so_far

        return slabs(m[i].at[l], body, jnp.zeros((ROWS, LANES), F32) if last else None)

    barrier = pltpu.get_barrier_semaphore()
    for other in (partner, away(0, 1) * CORES + core, come(0, 1) * CORES + core):
        pl.semaphore_signal(barrier, inc=1, device_id={"dp": other}, device_id_type=MESH)
    for i, l in chunks:
        stage(i, l).start()
        mine(i, l, 0).start()
    pl.semaphore_wait(barrier, 3)
    for i, l in chunks:
        stage(i, l).wait()
        pair(i, l, 0).start()

    moments = [pltpu.make_async_copy(src[i], dst[i], load_sem.at[i, k]) for i in range(3) for k, (src, dst) in enumerate(((m_in, m), (v_in, v)))]
    old = [pltpu.make_async_copy(weights[i].at[l, me], w[i].at[l], load_sem.at[i, 2 + l]) for i, l in chunks]

    for i, l in chunks:
        add(i, l, 0, True, False)
        send_total(i, l, 0).start()
    for i, l in chunks:
        pair(i, l, 1).start()
        mine(i, l, 1).start()
    for load in moments:
        load.start()

    @pl.loop(1, chips - 1)
    def _(s):
        for i, l in chunks:
            pair(i, l, s + 1).start()
            mine(i, l, s + 1).start()
        for i, l in chunks:
            add(i, l, s, False, False)
            send_total(i, l, s).start()

    for load in old:
        load.start()

    def sent(i, l, s):
        slot = whole[i][l].at[s]
        return remote(slot, slot, ring_send.at[i, l, s], ring_recv.at[i, l, s], away(l, 1) * CORES + core)

    @pl.loop(0, chips - 2)
    def _(s):
        for i, l in chunks:
            pair(i, l, s).wait_send()
            sent(i, l, s).wait_send()

    for i, l in chunks:
        pair(i, l, chips - 2).wait_send()
    square = jnp.zeros((ROWS, LANES), F32)
    for i, l in chunks:
        square += add(i, l, chips - 1, False, True)
    squares[me] = jnp.sum(square, axis=0, keepdims=True)
    for i, l in chunks:
        sent(i, l, chips - 2).wait_send()

    def norm(to, source):
        return remote(squares.at[source], squares.at[source], norm_send.at[to], norm_recv.at[source], to)

    for other in sorted(range(1, group), key=lambda other: abs(group // 2 - other)):
        norm(lax.rem(me + other, group), me).start()
    for i, l in chunks:
        pair(i, l, chips - 1).wait_send()
    for load in (*moments, *old):
        load.wait()
    for other in range(1, group):
        norm(lax.rem(me + other, group), lax.rem(me + other, group)).wait_recv()
    square = jnp.sum(jnp.sum(squares[...], axis=0), axis=1, keepdims=True)
    factor = jnp.minimum(1.0, 0.5 * lax.rsqrt(square / count + 1e-30))[None]

    def ring(i, l, s):
        slot = whole[i][l].at[come(l, s) * CORES + core]
        return remote(slot, slot, ring_send.at[i, l, s], ring_recv.at[i, l, s], away(l, 1) * CORES + core)

    def share(i, l, s):
        slot = whole[i][l].at[come(l, s) * CORES + core]
        return remote(slot, slot, pair_send.at[i, l, s], pair_recv.at[i, l, s], partner)

    for i, l in chunks:

        def body(at, so_far):
            new = adamw(w[i][l, at].astype(F32), m[i][l, at], v[i][l, at], g[i][l, at].astype(F32) * factor)
            whole[i][l][me, at], m[i][l, at], v[i][l, at] = new
            return so_far

        slabs(m[i].at[l], body)
        ring(i, l, 0).start()
        share(i, l, 0).start()

    @pl.loop(1, chips - 1)
    def _(s):
        for i, l in chunks:
            ring(i, l, s - 1).wait_recv()
            ring(i, l, s).start()
            share(i, l, s).start()

    for other in range(1, group):
        norm(lax.rem(me + other, group), me).wait_send()

    @pl.loop(0, chips - 2)
    def _(s):
        for i, l in chunks:
            ring(i, l, s).wait_send()
            share(i, l, s).wait_send()
            share(i, l, s).wait_recv()

    for i, l in chunks:
        ring(i, l, chips - 2).wait_recv()
        share(i, l, chips - 1).start()
    for s in (chips - 2, chips - 1):
        for i, l in chunks:
            if s < chips - 1:
                ring(i, l, s).wait_send()
            share(i, l, s).wait_send()
            share(i, l, s).wait_recv()


def write(layers, *refs):
    *refs, sem = refs
    src, dst = refs[:-9], refs[-9:]
    pieces = [(src[i * layers + l], dst[i].at[l]) for i in range(3) for l in range(layers)]
    pieces += zip(src[3 * layers :], dst[3:], strict=True)
    copies = [pltpu.make_async_copy(*piece, sem.at[i]) for i, piece in enumerate(pieces)]
    for copy in copies:
        copy.start()
    for copy in copies:
        copy.wait()


def solution(mesh):
    group = mesh.shape["dp"]
    chips = group // CORES

    def step(*arrays):
        terms, weights, m, v = (arrays[i : i + 3] for i in (0, 3, 6, 9))
        layers = terms[0].shape[1]
        chunk = [(one.shape[1] // ROWS, ROWS, one.shape[2]) for one in m]
        blocks = [(layers, group, *one) for one in chunk]
        local = [(layers, *one) for one in chunk]
        terms = [one.reshape(shape) for one, shape in zip(terms, blocks, strict=True)]
        old = [one.reshape(shape) for one, shape in zip(weights, blocks, strict=True)]
        moments = [one.reshape(shape) for one, shape in zip(m + v, local * 2, strict=True)]
        kept = [pltpu.VMEM(shape[1:], jnp.bfloat16) for shape in blocks for _ in range(layers)] + [pltpu.VMEM(shape, F32) for shape in local * 2]
        elements = sum(math.prod(shape) for shape in blocks)
        new = pl.pallas_call(
            kernel,
            out_shape=kept,
            in_specs=[pl.BlockSpec(memory_space=pltpu.HBM)] * 12,
            out_specs=[pl.BlockSpec(memory_space=pltpu.VMEM)] * len(kept),
            scratch_shapes=[
                *(pltpu.VMEM((2, *shape), jnp.bfloat16) for shape in local),
                pltpu.VMEM((group, 1, LANES), F32),
                *[pltpu.SemaphoreType.DMA((3, layers, chips))] * 4,
                pltpu.SemaphoreType.DMA((3, layers, 2)),
                pltpu.SemaphoreType.DMA((3, layers)),
                pltpu.SemaphoreType.DMA((3, 2 + layers)),
                *[pltpu.SemaphoreType.DMA((group,))] * 2,
            ],
            compiler_params=pltpu.CompilerParams(collective_id=0, has_side_effects=True, vmem_limit_bytes=8 * 2**20),
            cost_estimate=pl.CostEstimate(flops=20 * elements, bytes_accessed=4 * elements, transcendentals=elements // group),
        )(*terms, *old, *moments)
        out = pl.pallas_call(
            functools.partial(write, layers),
            out_shape=[jax.ShapeDtypeStruct(shape, jnp.bfloat16) for shape in blocks] + [jax.ShapeDtypeStruct(shape, F32) for shape in local * 2],
            in_specs=[pl.BlockSpec(memory_space=pl.ANY)] * len(kept),
            out_specs=[pl.BlockSpec(memory_space=pl.ANY)] * 9,
            scratch_shapes=[pltpu.SemaphoreType.DMA((len(kept),))],
            compiler_params=pltpu.CompilerParams(vmem_limit_bytes=8 * 2**20),
        )(*new)
        return tuple(one.reshape(like.shape) for one, like in zip(out, weights + m + v, strict=True))

    all_of, cut = P(None, None, None), P(None, "dp", None)
    return jax.shard_map(
        step,
        mesh=mesh,
        in_specs=(P(("rep", "dp"), None, None, None),) * 3 + (all_of,) * 3 + (cut,) * 6,
        out_specs=(P("rep", None, None),) * 3 + (P("rep", "dp", None),) * 6,
        check_vma=False,
    )
```

```python
import functools
import math

import jax
import jax.numpy as jnp
from jax import lax
from jax.experimental import pallas as pl
from jax.experimental.pallas import tpu as pltpu
from jax.sharding import PartitionSpec as P

MESH = pl.DeviceIdType.MESH
CORES = 2
ROWS, LANES = 8, 128
SLAB = 28
F32 = jnp.float32


def adamw(w, m, v, g):
    m = 0.9 * m + 0.1 * g
    v = 0.95 * v + 0.05 * g * g
    step = m * lax.rsqrt(v + 1e-8) + 0.1 * w
    return (w - 0.02 * step).astype(jnp.bfloat16), m, v


def slabs(ref, body, start=None):
    tiles, columns = ref.shape[0], ref.shape[2]
    size = math.gcd(tiles, max(1, SLAB * LANES // columns))
    return lax.fori_loop(0, tiles // size, lambda i, so_far: body(pl.ds(i * size, size), so_far), start)


def kernel(*refs):
    layers = refs[0].shape[0]
    inputs, flat, rest = refs[:12], refs[12 : 12 + 3 * layers], refs[12 + 3 * layers :]
    terms, weights, m_in, v_in = (inputs[i : i + 3] for i in range(0, 12, 3))
    whole = [flat[i : i + layers] for i in range(0, 3 * layers, layers)]
    m, v, own = (rest[i : i + 3] for i in range(0, 9, 3))
    squares, pair_send, pair_recv, ring_send, ring_recv, own_sem, stage_sem, load_sem, norm_send, norm_recv = rest[9:]
    group = terms[0].shape[1]
    chips = group // CORES
    count = group * sum(math.prod(one.shape) for one in m)
    end = (chips - 1) % 2
    g, w = ([one.at[slot] for one in own] for slot in (end, 1 - end))
    me = lax.axis_index("dp")
    core, z = lax.rem(me, CORES), lax.div(me, CORES)
    partner = z * CORES + (1 - core)
    chunks = [(i, l) for i in range(3) for l in range(layers)]

    def away(l, steps):
        return lax.rem(z + (steps if l % 2 == 0 else chips - steps), chips)

    def come(l, steps):
        return lax.rem(z + (chips - steps if l % 2 == 0 else steps), chips)

    def remote(src, dst, send, recv, device):
        return pltpu.make_async_remote_copy(src_ref=src, dst_ref=dst, send_sem=send, recv_sem=recv, device_id={"dp": device}, device_id_type=MESH)

    def stage(i, l):
        return pltpu.make_async_copy(terms[i].at[l, come(l, 1) * CORES + (1 - core)], whole[i][l].at[group - 1], stage_sem.at[i, l])

    def pair(i, l, s):
        first = isinstance(s, int) and s == 0
        return remote(whole[i][l].at[group - 1] if first else terms[i].at[l, come(l, s + 1) * CORES + (1 - core)], whole[i][l].at[s], pair_send.at[i, l, s], pair_recv.at[i, l, s], partner)

    def mine(i, l, s):
        return pltpu.make_async_copy(terms[i].at[l, come(l, s + 1) * CORES + core], own[i].at[lax.rem(s, 2), l], own_sem.at[i, l, lax.rem(s, 2)])

    def total(l, s):
        return chips + s - 1

    def send_total(i, l, s):
        src = s if isinstance(s, int) and s == 0 else total(l, s)
        return remote(whole[i][l].at[src], whole[i][l].at[total(l, s + 1)], ring_send.at[i, l, s], ring_recv.at[i, l, s], away(l, 1) * CORES + core)

    def add(i, l, s, first, last):
        if not first:
            send_total(i, l, s - 1).wait_recv()
        mine(i, l, s).wait()
        pair(i, l, s).wait_recv()

        def body(at, so_far):
            value = own[i][lax.rem(s, 2), l, at].astype(F32) + whole[i][l][s, at].astype(F32)
            if not first:
                value += whole[i][l][total(l, s), at].astype(F32)
            value = value.astype(jnp.bfloat16)
            if not last:
                whole[i][l][s if first else total(l, s), at] = value
                return so_far
            g[i][l, at] = value
            value = value.astype(F32)
            value = jnp.sum(value * value, axis=0)
            for column in range(0, value.shape[1], LANES):
                so_far += value[:, column : column + LANES]
            return so_far

        return slabs(m[i].at[l], body, jnp.zeros((ROWS, LANES), F32) if last else None)

    barrier = pltpu.get_barrier_semaphore()
    for other in (partner, away(0, 1) * CORES + core, come(0, 1) * CORES + core):
        pl.semaphore_signal(barrier, inc=1, device_id={"dp": other}, device_id_type=MESH)
    for i, l in chunks:
        stage(i, l).start()
        mine(i, l, 0).start()
    pl.semaphore_wait(barrier, 3)
    for i, l in chunks:
        stage(i, l).wait()
        pair(i, l, 0).start()

    moments = [pltpu.make_async_copy(src[i], dst[i], load_sem.at[i, k]) for i in range(3) for k, (src, dst) in enumerate(((m_in, m), (v_in, v)))]
    old = [pltpu.make_async_copy(weights[i].at[l, me], w[i].at[l], load_sem.at[i, 2 + l]) for i, l in chunks]

    for i, l in chunks:
        add(i, l, 0, True, False)
        send_total(i, l, 0).start()
    for i, l in chunks:
        pair(i, l, 1).start()
        mine(i, l, 1).start()
    for load in moments:
        load.start()

    @pl.loop(1, chips - 1)
    def _(s):
        for i, l in chunks:
            pair(i, l, s + 1).start()
            mine(i, l, s + 1).start()
        for i, l in chunks:
            add(i, l, s, False, False)
            send_total(i, l, s).start()

    for load in old:
        load.start()

    def sent(i, l, s):
        slot = whole[i][l].at[s]
        return remote(slot, slot, ring_send.at[i, l, s], ring_recv.at[i, l, s], away(l, 1) * CORES + core)

    @pl.loop(0, chips - 2)
    def _(s):
        for i, l in chunks:
            pair(i, l, s).wait_send()
            sent(i, l, s).wait_send()

    for i, l in chunks:
        pair(i, l, chips - 2).wait_send()
    square = jnp.zeros((ROWS, LANES), F32)
    for i, l in chunks:
        square += add(i, l, chips - 1, False, True)
    squares[me] = jnp.sum(square, axis=0, keepdims=True)
    for i, l in chunks:
        sent(i, l, chips - 2).wait_send()

    def norm(to, source):
        return remote(squares.at[source], squares.at[source], norm_send.at[to], norm_recv.at[source], to)

    for other in sorted(range(1, group), key=lambda other: abs(group // 2 - other)):
        norm(lax.rem(me + other, group), me).start()
    for i, l in chunks:
        pair(i, l, chips - 1).wait_send()
    for load in (*moments, *old):
        load.wait()
    for other in range(1, group):
        norm(lax.rem(me + other, group), lax.rem(me + other, group)).wait_recv()
    square = jnp.sum(jnp.sum(squares[...], axis=0), axis=1, keepdims=True)
    factor = jnp.minimum(1.0, 0.5 * lax.rsqrt(square / count + 1e-30))[None]

    def ring(i, l, s):
        slot = whole[i][l].at[come(l, s) * CORES + core]
        return remote(slot, slot, ring_send.at[i, l, s], ring_recv.at[i, l, s], away(l, 1) * CORES + core)

    def share(i, l, s):
        slot = whole[i][l].at[come(l, s) * CORES + core]
        return remote(slot, slot, pair_send.at[i, l, s], pair_recv.at[i, l, s], partner)

    for i, l in chunks:

        def body(at, so_far):
            new = adamw(w[i][l, at].astype(F32), m[i][l, at], v[i][l, at], g[i][l, at].astype(F32) * factor)
            whole[i][l][me, at], m[i][l, at], v[i][l, at] = new
            return so_far

        slabs(m[i].at[l], body)
        ring(i, l, 0).start()
        share(i, l, 0).start()

    @pl.loop(1, chips - 1)
    def _(s):
        for i, l in chunks:
            ring(i, l, s - 1).wait_recv()
            ring(i, l, s).start()
            share(i, l, s).start()

    for other in range(1, group):
        norm(lax.rem(me + other, group), me).wait_send()

    @pl.loop(0, chips - 2)
    def _(s):
        for i, l in chunks:
            ring(i, l, s).wait_send()
            share(i, l, s).wait_send()
            share(i, l, s).wait_recv()

    for i, l in chunks:
        ring(i, l, chips - 2).wait_recv()
        share(i, l, chips - 1).start()
    for s in (chips - 2, chips - 1):
        for i, l in chunks:
            if s < chips - 1:
                ring(i, l, s).wait_send()
            share(i, l, s).wait_send()
            share(i, l, s).wait_recv()


def write(layers, *refs):
    *refs, sem = refs
    src, dst = refs[:-9], refs[-9:]
    pieces = list(zip(src[3 * layers :], dst[3:], strict=True))
    pieces += [(src[i * layers + l], dst[i].at[l]) for i in range(3) for l in range(layers)]
    copies = [pltpu.make_async_copy(*piece, sem.at[i]) for i, piece in enumerate(pieces)]
    for copy in copies:
        copy.start()
    for copy in copies:
        copy.wait()


def solution(mesh):
    group = mesh.shape["dp"]
    chips = group // CORES

    def step(*arrays):
        terms, weights, m, v = (arrays[i : i + 3] for i in (0, 3, 6, 9))
        layers = terms[0].shape[1]
        chunk = [(one.shape[1] // ROWS, ROWS, one.shape[2]) for one in m]
        blocks = [(layers, group, *one) for one in chunk]
        local = [(layers, *one) for one in chunk]
        terms = [one.reshape(shape) for one, shape in zip(terms, blocks, strict=True)]
        old = [one.reshape(shape) for one, shape in zip(weights, blocks, strict=True)]
        moments = [one.reshape(shape) for one, shape in zip(m + v, local * 2, strict=True)]
        kept = [pltpu.VMEM(shape[1:], jnp.bfloat16) for shape in blocks for _ in range(layers)] + [pltpu.VMEM(shape, F32) for shape in local * 2]
        elements = sum(math.prod(shape) for shape in blocks)
        new = pl.pallas_call(
            kernel,
            out_shape=kept,
            in_specs=[pl.BlockSpec(memory_space=pltpu.HBM)] * 12,
            out_specs=[pl.BlockSpec(memory_space=pltpu.VMEM)] * len(kept),
            scratch_shapes=[
                *(pltpu.VMEM((2, *shape), jnp.bfloat16) for shape in local),
                pltpu.VMEM((group, 1, LANES), F32),
                *[pltpu.SemaphoreType.DMA((3, layers, chips))] * 4,
                pltpu.SemaphoreType.DMA((3, layers, 2)),
                pltpu.SemaphoreType.DMA((3, layers)),
                pltpu.SemaphoreType.DMA((3, 2 + layers)),
                *[pltpu.SemaphoreType.DMA((group,))] * 2,
            ],
            compiler_params=pltpu.CompilerParams(collective_id=0, has_side_effects=True, vmem_limit_bytes=8 * 2**20),
            cost_estimate=pl.CostEstimate(flops=20 * elements, bytes_accessed=4 * elements, transcendentals=elements // group),
        )(*terms, *old, *moments)
        out = pl.pallas_call(
            functools.partial(write, layers),
            out_shape=[jax.ShapeDtypeStruct(shape, jnp.bfloat16) for shape in blocks] + [jax.ShapeDtypeStruct(shape, F32) for shape in local * 2],
            in_specs=[pl.BlockSpec(memory_space=pl.ANY)] * len(kept),
            out_specs=[pl.BlockSpec(memory_space=pl.ANY)] * 9,
            scratch_shapes=[pltpu.SemaphoreType.DMA((len(kept),))],
            compiler_params=pltpu.CompilerParams(vmem_limit_bytes=8 * 2**20),
        )(*new)
        return tuple(one.reshape(like.shape) for one, like in zip(out, weights + m + v, strict=True))

    all_of, cut = P(None, None, None), P(None, "dp", None)
    return jax.shard_map(
        step,
        mesh=mesh,
        in_specs=(P(("rep", "dp"), None, None, None),) * 3 + (all_of,) * 3 + (cut,) * 6,
        out_specs=(P("rep", None, None),) * 3 + (P("rep", "dp", None),) * 6,
        check_vma=False,
    )
```
